256 devices in a mesh: ens: 4 (over y, x), region: 32 (over z), feat: 2 (over core).
Axes of the slice: x: 2, y: 2, z: 32, core: 2. Of those that a mesh axis runs over, the one named last changes fastest.
The devices are a block of a 4x8x32 slice.
Arguments:
- grid_lat: bfloat16 [131072, 512], P(('ens', 'region', 'feat')), parts along dimension 0, may hold values from -6 to 6
- g2m_edge: bfloat16 [262144, 512], P(('ens', 'region', 'feat')), parts along dimension 0, may hold values from -6 to 6
- g2m_src: int32 [262144], P(('ens', 'region', 'feat')), parts along dimension 0, may hold values from 0 to 32767, as said below
- g2m_owner: int32 [262144, 1], P(('ens', 'region', 'feat')), parts along dimension 0, may hold values from 0 to 63; in each aligned block of 1024 rows (0 to 1023, 1024 to 2047, ...) at most 32 rows name the same one
- g2m_row: int32 [262144], P(('ens', 'region', 'feat')), parts along dimension 0, may hold values from 0 to 255
- mesh_lat: bfloat16 [65536, 512], P(('ens', 'region', 'feat')), parts along dimension 0, may hold values from -6 to 6
- m2m_edge: bfloat16 [65536, 8, 512], P(('ens', 'region', 'feat')), parts along dimension 0, may hold values from -6 to 6
- m2m_src: int32 [65536, 8], P(('ens', 'region', 'feat')), parts along dimension 0, may hold values from 0 to 16383, as said below
- enc_edge_w: bfloat16 [4, 512, 512], P(None, None, 'feat'), may hold values from -0.25 to 0.25
- enc_node_w: bfloat16 [3, 512, 512], P(None, None, 'feat'), may hold values from -0.25 to 0.25
- proc_edge_w: bfloat16 [2, 4, 512, 512], P(None, None, None, 'feat'), may hold values from -0.25 to 0.25
- proc_node_w: bfloat16 [2, 3, 512, 512], P(None, None, None, 'feat'), may hold values from -0.25 to 0.25
Outputs:
- mesh_out: bfloat16 [65536, 512], P(('ens', 'region', 'feat')), parts along dimension 0
The draws below stay inside these ranges and needn't reach their ends.
There are 4 independent parts, one for each index of `ens`. The reference program is written for one: setup_inputs(seed, part) draws one part's arguments, and reference() takes and returns one part's arrays. A program takes and returns all parts, laid end to end along the dimension named above; an argument that names none is the same for every part. Nothing has to cross between parts.
Inputs may be any that keep to these rules, and one draw needn't show every extreme that they name: Edge i is sent by a grid node of block i // 1024, that is g2m_src[i] // 512 == i // 1024. `g2m_owner`: among the 1024 edges of one block, at most 32 have the same owner. `m2m_src`: for a receiving node v of block b = v // 256, every sender s has s % 256 < 8, or b * 256 - 128 <= s < (b + 1) * 256 + 128.
All inputs are finite; a program needn't handle non-finite values.
Results may differ from the reference program's by a relative error of at most 0.017.
Values may be sent and summed in bfloat16 or wider, within the bound.
No kernel may reach another device: no remote copies, remote signals or barrier semaphores. Data moves between devices by JAX's collectives and lax.ppermute only.
A program may use at most 128 MiB of HBM per device.

```python
import math
import jax
import jax.numpy as jnp
import numpy as np
from jax import lax

D = 512
GR_DEV = 512
MR_DEV = 256
MC_DEV = 8
KDEG = 8
LAYERS = 2
SHARDS = 64
E_DEV = 1024
CAP = 32
HALO = 128
NGRID = 32768
NMESH = 16384
NEDGE = 65536


def draw_g2m_src(key, part):
    inner = jax.random.fold_in(key, 31)
    edge_ids = jnp.arange(NEDGE, dtype=jnp.int32)
    offset = jax.random.randint(inner, (NEDGE,), 0, GR_DEV, dtype=jnp.int32)
    return (edge_ids // E_DEV * GR_DEV + offset).astype(jnp.int32)


def draw_m2m_src(key, part):
    inner = jax.random.fold_in(key, 57)
    first, second, third, fourth = jax.random.split(inner, 4)
    shape = (NMESH, KDEG)
    node_ids = jnp.arange(NMESH, dtype=jnp.int32)[:, None]
    block = node_ids // MR_DEV
    picker = jax.random.randint(first, shape, 0, 4, dtype=jnp.int32)
    far_block = jax.random.randint(second, shape, 0, SHARDS, dtype=jnp.int32)
    far_row = jax.random.randint(third, shape, 0, MC_DEV, dtype=jnp.int32)
    nearby = block * MR_DEV - HALO + jax.random.randint(fourth, shape, 0, MR_DEV + 2 * HALO, dtype=jnp.int32)
    nearby = jnp.clip(nearby, 0, NMESH - 1)
    return jnp.where(picker == 0, far_block * MR_DEV + far_row, nearby).astype(jnp.int32)


def touch_ends(values, own_key, least, top_value):
    longest = values.shape.index(max(values.shape))
    spots = []
    for shift in (0, 1):
        where = [jax.random.randint(jax.random.fold_in(own_key, axis), (), 0, length) for axis, length in enumerate(values.shape)]
        where[longest] = (where[longest] + shift) % values.shape[longest]
        spots.append(tuple(where))
    return values.at[spots[0]].set(least).at[spots[1]].set(top_value)


def shard_levels(key, extent, cuts, least, top_value):
    def one(dim, blocks):
        steps = jax.random.uniform(jax.random.fold_in(jax.random.fold_in(key, 6), dim), (blocks,), jnp.float32, least / len(cuts), top_value / len(cuts))
        return jnp.repeat(jnp.exp(steps), extent[dim] // blocks).reshape((-1,) + (1,) * (len(extent) - dim - 1))

    loudness = one(*cuts[0])
    for cut in cuts[1:]:
        loudness = loudness * one(*cut)
    return loudness


def assign_block(key, own, number, rows, count, top, bound, skew):
    sequence = jax.random.permutation(key, count)
    packed, common = load_shares(count, rows * top, bound, skew, True), load_shares(count, rows * top, bound, skew, False)
    places = jnp.arange(count)

    def named(tallies, offset_by):
        used = int((tallies > 0).sum())
        fixed = max(1, used // 4)
        moved = fixed + (places - fixed + offset_by * (used - fixed)) % max(1, count - fixed)
        return jnp.zeros((count,), jnp.int32).at[sequence[jnp.where(places < fixed, places, moved)]].set(jnp.asarray(tallies, jnp.int32))

    tallies = jnp.where(number % 4 == 0, named(packed, number // 4), named(common, number - number // 4 - 1))
    mixed = jax.random.permutation(jax.random.fold_in(own, 3), count)
    source_of, sink = mixed[0:count // 2 * 2:2], mixed[1:count // 2 * 2:2]
    margin = jnp.minimum(tallies[source_of] - 1, bound - tallies[sink]) // 2
    margin = jnp.where((source_of == sequence[0]) | (sink == sequence[0]) | (tallies[sink] == 0), 0, jnp.maximum(margin, 0))
    moved = jax.random.randint(jax.random.fold_in(own, 4), (count // 2,), 0, 1 << 20) % (margin + 1)
    tallies = tallies.at[source_of].add(-moved).at[sink].add(moved)
    members = jnp.searchsorted(jnp.cumsum(tallies), jnp.arange(rows * top), side="right").astype(jnp.int32)
    listing = members.reshape(top, rows).T
    listing = listing[jax.random.permutation(jax.random.fold_in(own, 1), rows)]
    offset_by = jax.random.randint(jax.random.fold_in(own, 2), (rows, 1), 0, top)
    return jnp.take_along_axis(listing, (jnp.arange(top)[None, :] + offset_by) % top, axis=1)


def load_shares(count, total, limit, lean, full):
    weights = [(1 << 20) // math.isqrt(standing ** lean) + 1 for standing in range(1, count + 1)]
    largest = limit if full else min(limit, max(-(-total // count), total * weights[0] // sum(weights)))
    least = 1 if total - largest >= count - 1 else 0
    holding, surplus = [largest] + [least] * (count - 1), total - largest - least * (count - 1)
    while surplus > 0:
        free = [i for i in range(1, count) if holding[i] < largest] or [i for i in range(1, count) if holding[i] < limit]
        whole, remaining = sum([weights[i] for i in free]), surplus
        for i in free:
            extra = min(limit - holding[i], max(1, remaining * weights[i] // whole), surplus)
            holding[i] = holding[i] + extra
            surplus = surplus - extra
    return np.array(holding)


def gaussian(stream_key, shape, scale, bound, cuts=(), kind=jnp.bfloat16):
    entries = scale * jax.random.normal(stream_key, shape, jnp.float32)
    if cuts:
        entries = entries * shard_levels(stream_key, shape, cuts, -0.22, 0.18)
    return jnp.clip(entries, -bound, bound).astype(kind)


def setup_inputs(seed: int = 0, part: int = 0) -> dict:
    streams_of = jax.random.split(jax.random.key(seed), 13)
    part_splits = jax.random.split(jax.random.fold_in(streams_of[12], part), 13)
    grid_lat = gaussian(part_splits[0], (NGRID, D), 1.0, 6.0, ((0, 64),))
    g2m_edge = gaussian(part_splits[1], (NEDGE, D), 1.0, 6.0, ((0, 64),))
    g2m_src = draw_g2m_src(jax.random.fold_in(jax.random.fold_in(streams_of[12], part), 71), part)
    g2m_owner_keys = jax.random.split(jax.random.fold_in(part_splits[3], 1), NEDGE // E_DEV)
    g2m_owner_turns = jax.random.permutation(jax.random.fold_in(part_splits[3], 3), NEDGE // E_DEV)
    g2m_owner = jax.vmap(lambda own, number: assign_block(jax.random.fold_in(part_splits[3], 2), own, number, E_DEV, SHARDS, 1, CAP, 2))(g2m_owner_keys, g2m_owner_turns).reshape((NEDGE, 1))
    g2m_row = touch_ends(jax.random.randint(part_splits[4], (NEDGE,), 0, MR_DEV), jax.random.fold_in(part_splits[4], 1), 0, MR_DEV - 1).astype(jnp.int32)
    mesh_lat = gaussian(part_splits[5], (NMESH, D), 1.0, 6.0, ((0, 64),))
    m2m_edge = gaussian(part_splits[6], (NMESH, KDEG, D), 1.0, 6.0, ((0, 64),))
    m2m_src = draw_m2m_src(jax.random.fold_in(jax.random.fold_in(streams_of[12], part), 71), part)
    enc_edge_w = gaussian(streams_of[8], (4, D, D), D ** -0.5, 0.25, ((2, 2),))
    enc_node_w = gaussian(streams_of[9], (3, D, D), D ** -0.5, 0.25, ((2, 2),))
    proc_edge_w = gaussian(streams_of[10], (LAYERS, 4, D, D), D ** -0.5, 0.25, ((3, 2),))
    proc_node_w = gaussian(streams_of[11], (LAYERS, 3, D, D), D ** -0.5, 0.25, ((3, 2),))
    return {"grid_lat": grid_lat, "g2m_edge": g2m_edge, "g2m_src": g2m_src, "g2m_owner": g2m_owner, "g2m_row": g2m_row, "mesh_lat": mesh_lat, "m2m_edge": m2m_edge, "m2m_src": m2m_src, "enc_edge_w": enc_edge_w, "enc_node_w": enc_node_w, "proc_edge_w": proc_edge_w, "proc_node_w": proc_node_w}


def layer_norm(values):
    center = values - lax.optimization_barrier(jnp.mean(values, axis=-1, keepdims=True))
    spread = lax.optimization_barrier(jnp.mean(center * center, axis=-1, keepdims=True))
    return center * lax.rsqrt(spread + 1e-05)

def project(latent, matrix):
    return jnp.dot(latent, matrix, preferred_element_type=jnp.float32).astype(jnp.bfloat16)

def edge_output(pre_act, matrix):
    hidden = jax.nn.silu(pre_act).astype(jnp.bfloat16)
    return layer_norm(jnp.dot(hidden, matrix, preferred_element_type=jnp.float32)).astype(jnp.bfloat16)

def node_update(latent, aggregate, stack):
    pre_act = jnp.dot(latent, stack[0], preferred_element_type=jnp.float32)
    pre_act = pre_act + jnp.dot(aggregate, stack[1], preferred_element_type=jnp.float32)
    hidden = jax.nn.silu(pre_act).astype(jnp.bfloat16)
    update = layer_norm(jnp.dot(hidden, stack[2], preferred_element_type=jnp.float32))
    return (latent.astype(jnp.float32) + update).astype(jnp.bfloat16)

def reference(grid_lat, g2m_edge, g2m_src, g2m_owner, g2m_row, mesh_lat, m2m_edge, m2m_src, enc_edge_w, enc_node_w, proc_edge_w, proc_node_w):
    sender = project(grid_lat, enc_edge_w[1])
    receiver = project(mesh_lat, enc_edge_w[2])
    target = (g2m_owner[:, 0] * MR_DEV + g2m_row).astype(jnp.int32)
    partial_sum = jnp.dot(g2m_edge, enc_edge_w[0], preferred_element_type=jnp.float32)
    partial_sum = (partial_sum + sender[g2m_src].astype(jnp.float32)).astype(jnp.bfloat16)
    pre_act = partial_sum.astype(jnp.float32) + receiver[target].astype(jnp.float32)
    message = edge_output(pre_act, enc_edge_w[3])
    aggregate = jax.ops.segment_sum(message.astype(jnp.float32), target, num_segments=NMESH)
    mesh = node_update(mesh_lat, aggregate.astype(jnp.bfloat16), enc_node_w)
    edges = m2m_edge.reshape(NMESH * KDEG, D)
    senders = m2m_src.reshape(NMESH * KDEG)
    for layer in range(LAYERS):
        edge_stack = proc_edge_w[layer]
        node_stack = proc_node_w[layer]
        sender = project(mesh, edge_stack[1])
        receiver = project(mesh, edge_stack[2])
        pre_act = jnp.dot(edges, edge_stack[0], preferred_element_type=jnp.float32)
        pre_act = pre_act + sender[senders].astype(jnp.float32) + jnp.repeat(receiver, KDEG, axis=0).astype(jnp.float32)
        message = edge_output(pre_act, edge_stack[3])
        aggregate = lax.optimization_barrier(jnp.sum(message.astype(jnp.float32).reshape(NMESH, KDEG, D), axis=1))
        edges = (edges.astype(jnp.float32) + message.astype(jnp.float32)).astype(jnp.bfloat16)
        mesh = node_update(mesh, aggregate.astype(jnp.bfloat16), node_stack)
    return mesh
```

```python
import functools

import jax
import jax.numpy as jnp
from jax import lax
from jax.experimental import pallas as pl
from jax.experimental.pallas import tpu as pltpu
from jax.sharding import PartitionSpec as P

MC_DEV = 8
BF = jnp.bfloat16
F32 = jnp.float32
I32 = jnp.int32
AXES = ("region", "feat")


def mm(a, b):
    return jnp.dot(a, b, preferred_element_type=F32)


def iota(shape, dim):
    return lax.broadcasted_iota(I32, shape, dim)


def mask(cond):
    return jnp.where(cond, 1.0, 0.0).astype(BF)


def silu(x):
    h = 0.5 * x
    return h + h * jnp.tanh(h)


def norm(y):
    center = y - jnp.mean(y, axis=-1, keepdims=True)
    spread = jnp.mean(center * center, axis=-1, keepdims=True)
    return center * lax.rsqrt(spread + 1e-05)


def join(feat_ref, own, other, out):
    half = own.shape[-1]

    @pl.when(feat_ref[0] == 0)
    def _():
        out[:, :half] = own[...]
        out[:, half:] = other[...]

    @pl.when(feat_ref[0] != 0)
    def _():
        out[:, :half] = other[...]
        out[:, half:] = own[...]


def node_update(latent, aggregate, wn):
    pre = mm(latent, wn[0]) + mm(aggregate, wn[1])
    update = norm(mm(silu(pre).astype(BF), wn[2]))
    return (latent.astype(F32) + update).astype(BF)


def slots_kernel(shards, chunk, owner_ref, row_ref, slot_ref, rows_ref):
    edges = owner_ref.shape[1]
    owner = owner_ref[...]
    step = 128
    tri = mask(iota((step, step), 0) <= iota((step, step), 1))
    carry = jnp.zeros((shards, 1), F32)
    ranks = []
    for b in range(edges // step):
        hot = iota((shards, step), 0) == owner[:, b * step : (b + 1) * step]
        count = mm(mask(hot), tri) + carry
        ranks.append(jnp.sum(jnp.where(hot, count, 0.0), axis=0, keepdims=True))
        carry = count[:, step - 1 :]
    rank = jnp.concatenate(ranks, axis=1).astype(I32) - 1
    slot = (rank // chunk) * (shards * chunk) + owner * chunk + rank % chunk
    slot_ref[...] = slot
    value = jnp.broadcast_to((row_ref[...] + 1).astype(F32), (8, edges)).astype(BF)
    width = 256
    for j in range(rows_ref.shape[1] // width):
        pick = mask(iota((width, edges), 0) + j * width == slot)
        got = lax.dot_general(value, pick, (((1,), (1,)), ((), ())), preferred_element_type=F32)
        rows_ref[:, j * width : (j + 1) * width] = got[0:1].astype(I32) - 1


def pack_kernel(feat_ref, grid_ref, edge_ref, src_ref, slot_ref, own_ref, oth_ref, *refs):
    outs, (w, partial) = refs[:-2], refs[-2:]
    for k in range(2):
        join(feat_ref, own_ref.at[k], oth_ref.at[k], w.at[k])
    sender = mm(grid_ref[...], w[1]).astype(BF)
    rows = 512
    edges = edge_ref.shape[0]
    for b in range(edges // rows):
        sl = pl.ds(b * rows, rows)
        pick = mask(iota((rows, sender.shape[0]), 1) == src_ref[sl, :])
        partial[sl, :] = (mm(edge_ref[sl, :], w[0]) + mm(pick, sender)).astype(BF)
    base = 0
    for out in outs:
        total = out.shape[0]
        for b in range(total // rows):
            pick = mask(iota((rows, edges), 0) + (base + b * rows) == slot_ref[...])
            out[b * rows : (b + 1) * rows, :] = mm(pick, partial[...]).astype(BF)
        base += total


def encode_kernel(feat_ref, *refs):
    nch = (len(refs) - 16) // 1
    gots = refs[:nch]
    (tcol_ref, trow_ref, mesh_ref, we_own, we_oth, wn_own, wn_oth, pe_own, pe_oth) = refs[nch : nch + 9]
    out_mesh, out_send, out_recv, we, wn, pe, agg = refs[nch + 9 :]
    for k in range(2):
        join(feat_ref, we_own.at[k + 2], we_oth.at[k + 2], we.at[k])
        join(feat_ref, pe_own.at[k + 1], pe_oth.at[k + 1], pe.at[k])
    for k in range(3):
        join(feat_ref, wn_own.at[k], wn_oth.at[k], wn.at[k])
    mesh = mesh_ref[...]
    mesh_rows = mesh.shape[0]
    recv = mm(mesh, we[0]).astype(BF)
    rows = 512
    base = 0
    first = True
    for got in gots:
        for b in range(got.shape[0] // rows):
            sl = pl.ds(base, rows)
            pick = mask(iota((rows, mesh_rows), 1) == tcol_ref[sl, :])
            pre = got[b * rows : (b + 1) * rows, :].astype(F32) + mm(pick, recv)
            msg = norm(mm(silu(pre).astype(BF), we[1])).astype(BF)
            put = mask(iota((mesh_rows, rows), 0) == trow_ref[:, sl])
            part = mm(put, msg)
            agg[...] = part if first else agg[...] + part
            first = False
            base += rows
    new = node_update(mesh, agg[...].astype(BF), wn)
    out_mesh[...] = new
    out_send[...] = mm(new, pe[0]).astype(BF)
    out_recv[...] = mm(new, pe[1]).astype(BF)


def layer_kernel(kdeg, last, feat_ref, edge_ref, index_ref, send_ref, low_ref, high_ref, coarse_ref,
                 recv_ref, mesh_ref, we_own, we_oth, wn_own, wn_oth, *refs):
    if last:
        out_mesh, we, wn, table, agg = refs
    else:
        pe_own, pe_oth, out_mesh, out_edge, out_send, out_recv, we, wn, table, agg, pe = refs
        for k in range(2):
            join(feat_ref, pe_own.at[k + 1], pe_oth.at[k + 1], pe.at[k])
    join(feat_ref, we_own.at[0], we_oth.at[0], we.at[0])
    join(feat_ref, we_own.at[3], we_oth.at[3], we.at[1])
    for k in range(3):
        join(feat_ref, wn_own.at[k], wn_oth.at[k], wn.at[k])
    at = 0
    for part in (low_ref, send_ref, high_ref, coarse_ref):
        table[at : at + part.shape[0], :] = part[...]
        at += part.shape[0]
    rows = 512
    group = rows // kdeg
    spread = mask(iota((rows, group), 0) // kdeg == iota((rows, group), 1))
    gather = mask(iota((group, rows), 0) == iota((group, rows), 1) // kdeg)
    for b in range(edge_ref.shape[0] // rows):
        sl = pl.ds(b * rows, rows)
        gl = pl.ds(b * group, group)
        edge = edge_ref[sl, :]
        pick = mask(iota((rows, at), 1) == index_ref[sl, :])
        pre = mm(edge, we[0]) + mm(pick, table[...]) + mm(spread, recv_ref[gl, :])
        msg = norm(mm(silu(pre).astype(BF), we[1])).astype(BF)
        if not last:
            out_edge[sl, :] = (edge.astype(F32) + msg.astype(F32)).astype(BF)
        agg[gl, :] = mm(gather, msg).astype(BF)
    new = node_update(mesh_ref[...], agg[...], wn)
    out_mesh[...] = new
    if not last:
        out_send[...] = mm(new, pe[0]).astype(BF)
        out_recv[...] = mm(new, pe[1]).astype(BF)


def call(kernel, feat, args, outs, scratch, name):
    vmem = pl.BlockSpec(memory_space=pltpu.VMEM)
    return pl.pallas_call(
        kernel,
        in_specs=[pl.BlockSpec(memory_space=pltpu.SMEM)] * (feat is not None) + [vmem] * len(args),
        out_specs=[vmem] * len(outs),
        out_shape=[jax.ShapeDtypeStruct(s, d) for s, d in outs],
        scratch_shapes=[pltpu.VMEM(s, d) for s, d in scratch],
        compiler_params=pltpu.CompilerParams(vmem_limit_bytes=56 * 1024 * 1024),
        name=name,
    )(*([feat] if feat is not None else []), *args)


def swap(stack):
    return lax.ppermute(stack, "feat", [(0, 1), (1, 0)])


def on_device(
    grid_lat, g2m_edge, g2m_src, g2m_owner, g2m_row, mesh_lat, m2m_edge, m2m_src,
    enc_edge_w, enc_node_w, proc_edge_w, proc_node_w, *, chunks,
):
    shards = lax.axis_size(AXES)
    myself = lax.axis_index(AXES)
    feat = lax.axis_index("feat").astype(I32).reshape(1)
    grid_rows, width = grid_lat.shape
    mesh_rows = mesh_lat.shape[0]
    edges = g2m_edge.shape[0]
    capacity = 2 * edges // shards
    slot_total = shards * capacity
    chunk = capacity // chunks
    layers = proc_edge_w.shape[0]

    slot, row_slots = call(
        functools.partial(slots_kernel, shards, chunk), None,
        [g2m_owner.reshape(1, edges), g2m_row.reshape(1, edges)],
        [((1, edges), I32), ((1, slot_total), I32)], [], "slots",
    )
    enc_edge_o = swap(enc_edge_w)
    row_slots = row_slots.reshape(chunks, shards, chunk).transpose(1, 0, 2).reshape(shards, capacity)
    targets = lax.all_to_all(row_slots, AXES, split_axis=0, concat_axis=0, tiled=True)
    targets = targets.reshape(shards, chunks, chunk).transpose(1, 0, 2).reshape(slot_total)
    enc_node_o = swap(enc_node_w)
    proc_edge_o = swap(proc_edge_w)
    proc_node_o = swap(proc_node_w)

    local_src = (g2m_src - myself * grid_rows).reshape(edges, 1)
    packed = call(
        pack_kernel, feat,
        [grid_lat, g2m_edge, local_src, slot, enc_edge_w, enc_edge_o],
        [((shards * chunk, width), BF)] * chunks,
        [((2, width, width), BF), ((edges, width), BF)], "pack",
    )
    gots = [
        lax.all_to_all(p.reshape(shards, chunk, width), AXES, split_axis=0, concat_axis=0, tiled=True)
        .reshape(shards * chunk, width)
        for p in packed
    ]
    mat = (width, width)
    mesh, sender, receiver = call(
        encode_kernel, feat,
        [*gots, targets.reshape(slot_total, 1), targets.reshape(1, slot_total), mesh_lat,
         enc_edge_w, enc_edge_o, enc_node_w, enc_node_o, proc_edge_w[0], proc_edge_o[0]],
        [((mesh_rows, width), BF)] * 3,
        [((2, *mat), BF), ((3, *mat), BF), ((2, *mat), BF), ((mesh_rows, width), F32)], "encode",
    )
    kdeg = m2m_src.shape[1]
    halo = mesh_rows // 2
    senders = m2m_src.reshape(mesh_rows * kdeg)
    home = senders // mesh_rows
    inside = senders % mesh_rows
    index = jnp.where(
        inside < MC_DEV,
        mesh_rows + 2 * halo + home * MC_DEV + inside,
        senders - (myself * mesh_rows - halo),
    ).reshape(mesh_rows * kdeg, 1)
    edge = m2m_edge.reshape(mesh_rows * kdeg, width)
    up = [(i, i + 1) for i in range(shards - 1)]
    for layer in range(layers):
        last = layer == layers - 1
        coarse = lax.all_gather(sender[:MC_DEV], AXES, tiled=True)
        low = lax.ppermute(sender[mesh_rows - halo :], AXES, up)
        high = lax.ppermute(sender[:halo], AXES, [(b, a) for a, b in up])
        args = [edge, index, sender, low, high, coarse, receiver, mesh,
                proc_edge_w[layer], proc_edge_o[layer], proc_node_w[layer], proc_node_o[layer]]
        outs = [((mesh_rows, width), BF)]
        scratch = [((2, *mat), BF), ((3, *mat), BF),
                   ((mesh_rows + 2 * halo + shards * MC_DEV, width), BF), ((mesh_rows, width), BF)]
        if not last:
            args += [proc_edge_w[layer + 1], proc_edge_o[layer + 1]]
            outs += [((mesh_rows * kdeg, width), BF)] + [((mesh_rows, width), BF)] * 2
            scratch += [((2, *mat), BF)]
        got = call(functools.partial(layer_kernel, kdeg, last), feat, args, outs, scratch, "layer")
        mesh = got[0]
        if not last:
            edge, sender, receiver = got[1:]
    return mesh


def solution(mesh):
    rows = P(("ens", "region", "feat"))
    rows2 = P(("ens", "region", "feat"), None)
    return jax.shard_map(
        functools.partial(on_device, chunks=2),
        mesh=mesh,
        in_specs=(
            rows2, rows2, rows, rows2, rows, rows2,
            P(("ens", "region", "feat"), None, None), rows2,
            P(None, None, "feat"), P(None, None, "feat"),
            P(None, None, None, "feat"), P(None, None, None, "feat"),
        ),
        out_specs=rows2,
        check_vma=False,
    )
```

```python
import functools

import jax
import jax.numpy as jnp
import numpy as np
from jax import lax
from jax.experimental import pallas as pl
from jax.experimental.pallas import tpu as pltpu
from jax.sharding import PartitionSpec as P

MC_DEV = 8
BF = jnp.bfloat16
F32 = jnp.float32
I32 = jnp.int32
AXES = ("region", "feat")
LANES = 128
SPAN = 1024
REGION = 1024
HEAD = 8
LIMIT = (1.09375, 104.0)


def mm(a, b):
    return jnp.dot(a, b, preferred_element_type=F32)


def iota(shape, dim):
    return lax.broadcasted_iota(I32, shape, dim)


def mask(cond):
    return jnp.where(cond, 1.0, 0.0).astype(BF)


def silu(x):
    h = 0.5 * x
    return h + h * jnp.tanh(h)


def norm(y):
    center = y - jnp.mean(y, axis=-1, keepdims=True)
    spread = jnp.mean(center * center, axis=-1, keepdims=True)
    return center * lax.rsqrt(spread + 1e-05)


def join(f, own, other, out):
    half = own.shape[-1]

    @pl.when(f == 0)
    def _():
        out[:, :half] = own[...]
        out[:, half:] = other[...]

    @pl.when(f != 0)
    def _():
        out[:, :half] = other[...]
        out[:, half:] = own[...]


def node_update(latent, aggregate, wn):
    pre = mm(latent, wn[0]) + mm(aggregate, wn[1])
    update = norm(mm(silu(pre).astype(BF), wn[2]))
    return (latent.astype(F32) + update).astype(BF)


def limits(n, cap, edges):
    held = []
    for hop in range(1, n // 2 + 1):
        left = n // 2 + 1 - hop
        held.append(min(2 * cap * left, -(-int(edges / n * left * LIMIT[0] + LIMIT[1]) // 8) * 8))
    return held


def route(owner, n, z, up):
    home, core = owner // 2, owner % 2
    ahead = jnp.where(home >= z, home - z, home - z + n)
    local = ahead == 0
    plus = (ahead < n // 2) | ((ahead == n // 2) & up)
    hops = jnp.where(plus, ahead, n - ahead)
    stream = jnp.where(local, 2, jnp.where(plus, 0, 1))
    key = jnp.where(local, 0, n // 2 - hops) * 2 + core
    return stream, key, hops


def slots_kernel(n, cap, widths, at_ref, owner_ref, row_ref, limit_ref, slot_ref, plain_ref, head_ref):
    z = at_ref[0]
    shards = 2 * n
    edges = owner_ref.shape[1]
    owner = owner_ref[...]
    step = LANES
    tri = mask(iota((step, step), 0) <= iota((step, step), 1))
    carry = jnp.zeros((shards, 1), F32)
    hots, ranks = [], []
    for b in range(edges // step):
        hot = iota((shards, step), 0) == owner[:, b * step : (b + 1) * step]
        count = mm(mask(hot), tri) + carry
        ranks.append(jnp.sum(jnp.where(hot, count, 0.0), axis=0, keepdims=True) - 1.0)
        hots.append(hot)
        carry = count[:, step - 1 :]
    ahead = iota((shards, 1), 0) // 2 - z
    ahead = jnp.where(ahead < 0, ahead + n, ahead)
    lean = jnp.where(ahead < n // 2, carry, jnp.where(ahead > n // 2, -carry, 0.0))
    lean = jnp.sum(jnp.where(ahead == 0, 0.0, lean), axis=0, keepdims=True)
    up = lean <= 0.0
    stream, key, hops = route(iota((shards, 1), 0), n, z, up)
    stream_r, key_r, _ = route(iota((1, shards), 1), n, z, up)
    before = mask((stream == stream_r) & (key_r < key))
    wide = jnp.broadcast_to(carry, (shards, LANES))
    start = mm(before, wide.astype(BF))[:, :1]
    start = jnp.where(stream == 2, (key * cap).astype(F32), start) + (stream * REGION).astype(F32)
    base = jnp.concatenate(
        [jnp.sum(jnp.where(h, start, 0.0), axis=0, keepdims=True) for h in hots], axis=1
    )
    rank = jnp.concatenate(ranks, axis=1)
    slot = (base + rank).astype(I32)
    slot_ref[...] = slot
    plain_ref[...] = owner * cap + rank.astype(I32)
    lane = iota((shards, LANES), 1)
    over = jnp.zeros((1, LANES), F32)
    for r in range(2):
        held = jnp.sum(jnp.where((stream == r) & (hops >= lane), wide, 0.0), axis=0, keepdims=True)
        over = jnp.maximum(over, jnp.where(held > limit_ref[r : r + 1, :].astype(F32), 1.0, 0.0))
    over = jnp.max(over, axis=1, keepdims=True)
    value = jnp.broadcast_to(row_ref[...].astype(F32), (HEAD, edges)).astype(BF)
    half = SPAN // 2
    line = iota((HEAD, half), 0)
    for r in range(3):
        parts = []
        for j in range(0, widths[r], LANES):
            pick = mask(iota((LANES, edges), 0) + (r * REGION + j) == slot)
            parts.append(lax.dot_general(value, pick, (((1,), (1,)), ((), ())), preferred_element_type=F32))
        if widths[r] < SPAN:
            parts.append(jnp.zeros((HEAD, SPAN - widths[r]), F32))
        targets = jnp.concatenate(parts, axis=1)
        counts = jnp.sum(jnp.where((stream == r) & (key == lane), wide, 0.0), axis=0, keepdims=True)
        counts = jnp.concatenate([counts, jnp.zeros((1, half - LANES), F32)], axis=1)
        head = jnp.where(line == 1, counts, jnp.where(line == 2, over, 0.0))
        head = jnp.where(line == 0, targets[:, :half], jnp.where(line == 3, targets[:, half:], head))
        head_ref[r] = head.astype(BF)


def pack_kernel(bases, plain, at_ref, grid_ref, edge_ref, src_ref, slot_ref, head_ref, own_ref, oth_ref, *refs):
    outs, (w, partial) = refs[:-2], refs[-2:]
    f = at_ref[1]
    for k in range(2):
        join(f, own_ref.at[k], oth_ref.at[k], w.at[k])
    sender = mm(grid_ref[...], w[1]).astype(BF)
    rows = 512
    edges, width = edge_ref.shape
    for b in range(edges // rows):
        sl = pl.ds(b * rows, rows)
        pick = mask(iota((rows, sender.shape[0]), 1) == src_ref[sl, :])
        partial[sl, :] = (mm(edge_ref[sl, :], w[0]) + mm(pick, sender)).astype(BF)
    if plain:
        (out,) = outs
        for b in range(out.shape[0] // rows):
            here = iota((rows, edges), 0) + b * rows == slot_ref[...]
            out[b * rows : (b + 1) * rows, :width] = mm(mask(here), partial[...]).astype(BF)
            target = jnp.sum(jnp.where(here, head_ref[...].astype(F32) + 1.0, 0.0), axis=1, keepdims=True) - 1.0
            out[b * rows : (b + 1) * rows, width:] = jnp.broadcast_to(target, (rows, LANES)).astype(BF)
        return
    half = width // 2
    for r, base in enumerate(bases):
        left, right = outs[2 * r], outs[2 * r + 1]
        total = right.shape[0]
        left[:HEAD, :] = head_ref[r, :, :half]
        left[HEAD : 2 * HEAD, :] = head_ref[r, :, half:]
        pick = mask(iota((total, edges), 0) + base == slot_ref[...])
        rows = mm(pick, partial[...]).astype(BF)
        left[2 * HEAD :, :] = rows[:, :half]
        right[...] = rows[:, half:]


def windows_kernel(n, cap, plan, pieces, at_ref, *refs):
    total = len(plan)
    starts = [sum(pieces[:i]) for i in range(total)]
    mine, other, heads, off_v, off_s, sems, hsems, osem = refs[sum(pieces) :]
    half = heads.shape[-1]
    held = [refs[s].shape[0] - 2 * HEAD for s in starts]
    f = at_ref[1]

    def head(i):
        return pltpu.make_async_copy(refs[starts[i]].at[pl.ds(0, 2 * HEAD), pl.ds(0, half)], heads.at[i], hsems.at[i])

    for i in range(total):
        head(i).start()
    for i in range(total):
        head(i).wait()
    lane = iota((1, LANES), 1)
    size = cap + 8
    over = jnp.zeros((1, 1), F32)
    spans = []
    for i, (first, local) in enumerate(plan):
        over = jnp.maximum(over, heads[i, 2:3, :1].astype(F32))
        counts = heads[i, 1:2, :LANES].astype(F32)
        for side, core in enumerate((f, 1 - f)):
            key = first + core
            if local:
                off = (core * cap).astype(F32) + jnp.zeros((1, 1), F32)
            else:
                off = jnp.sum(jnp.where(lane < key, counts, 0.0), axis=1, keepdims=True)
            num = jnp.sum(jnp.where(lane == key, counts, 0.0), axis=1, keepdims=True)
            limit = held[i] - size
            start = jnp.minimum(off.astype(I32) // 8, limit // 8) * 8
            spans.append((start, off, num))
            off_v[2 * i + side : 2 * i + side + 1, :] = jnp.broadcast_to(start, (1, LANES))
    copy = pltpu.make_async_copy(off_v, off_s, osem)
    copy.start()
    copy.wait()

    def fetch(i, side, part):
        out = (mine, other)[side]
        row = off_s[2 * i + side, 0] + (2 * HEAD if part == 0 else 0)
        cols = refs[starts[i]].shape[1]
        source = refs[starts[i] + part].at[pl.ds(pl.multiple_of(row, 8), size)]
        sink = out.at[pl.ds(i * size, size), pl.ds(part * half, cols)]
        return pltpu.make_async_copy(source, sink, sems.at[i, 2 * side + part])

    every = [(i, side, part) for i in range(total) for side in range(2) for part in range(pieces[i])]
    for each in every:
        fetch(*each).start()
    for i in range(total):
        targets = [heads[i, r : r + 1, :].astype(F32) for r in (0, HEAD, 3, HEAD + 3)]
        targets = jnp.concatenate(targets, axis=1)[:, : -(-held[i] // LANES) * LANES]
        span = (size, targets.shape[1])
        for side in range(2):
            start, off, num = spans[2 * i + side]
            place = iota(span, 0) + start
            value = jnp.sum(jnp.where(iota(span, 1) == place, targets, 0.0), axis=1, keepdims=True)
            at = (iota((size, 1), 0) + start).astype(F32)
            value = jnp.where((at >= off) & (at < off + num), value, -1.0)
            (mine, other)[side][i * size : (i + 1) * size, 2 * half :] = jnp.broadcast_to(value, (size, LANES)).astype(BF)
    tail = total * size
    for out in (mine, other):
        rest = out.shape[0] - tail
        out[tail:, : 2 * half] = jnp.broadcast_to(over, (rest, 2 * half)).astype(BF)
        out[tail:, 2 * half :] = jnp.full((rest, LANES), -1.0, BF)
    for each in every:
        fetch(*each).wait()


def encode_kernel(count, at_ref, *refs):
    gots = refs[:count]
    mesh_ref, we_own, we_oth, wn_own, wn_oth, pe_own, pe_oth = refs[count : count + 7]
    out_mesh, out_send, out_recv, we, wn, pe, agg = refs[count + 7 :]
    f = at_ref[1]
    for k in range(2):
        join(f, we_own.at[k + 2], we_oth.at[k + 2], we.at[k])
        join(f, pe_own.at[0, k + 1], pe_oth.at[0, k + 1], pe.at[k])
    for k in range(3):
        join(f, wn_own.at[k], wn_oth.at[k], wn.at[k])
    mesh = mesh_ref[...]
    mesh_rows, width = mesh.shape
    recv = mm(mesh, we[0]).astype(BF)
    first = True
    for got in gots:
        total = got.shape[0]
        rows = max(r for r in range(16, 513, 16) if total % r == 0)
        for b in range(total // rows):
            sl = pl.ds(b * rows, rows)
            target = got[sl, width:].astype(F32).astype(I32)
            pick = jnp.concatenate(
                [mask(iota((rows, LANES), 1) + c == target) for c in range(0, mesh_rows, LANES)], axis=1
            )
            pre = got[sl, :width].astype(F32) + mm(pick, recv)
            msg = norm(mm(silu(pre).astype(BF), we[1])).astype(BF)
            part = lax.dot_general(pick, msg, (((0,), (0,)), ((), ())), preferred_element_type=F32)
            agg[...] = part if first else agg[...] + part
            first = False
    new = node_update(mesh, agg[...].astype(BF), wn)
    out_mesh[...] = new
    out_send[...] = mm(new, pe[0]).astype(BF)
    out_recv[...] = mm(new, pe[1]).astype(BF)


def layer_kernel(kdeg, layer, last, pieces, at_ref, edge_ref, index_ref, send_ref, low_ref, high_ref, *refs):
    coarse, refs = refs[:pieces], refs[pieces:]
    recv_ref, mesh_ref, pe_own, pe_oth, wn_own, wn_oth, *refs = refs
    f = at_ref[1]
    if last:
        out_mesh, we, wn, table, agg = refs
    else:
        out_mesh, out_edge, out_send, out_recv, we, wn, table, agg, pe = refs
        for k in range(2):
            join(f, pe_own.at[layer + 1, k + 1], pe_oth.at[layer + 1, k + 1], pe.at[k])
    join(f, pe_own.at[layer, 0], pe_oth.at[layer, 0], we.at[0])
    join(f, pe_own.at[layer, 3], pe_oth.at[layer, 3], we.at[1])
    for k in range(3):
        join(f, wn_own.at[layer, k], wn_oth.at[layer, k], wn.at[k])
    at = 0
    for part in (low_ref, send_ref, high_ref, *coarse):
        table[at : at + part.shape[0], :] = part[...]
        at += part.shape[0]
    rows = 512
    group = rows // kdeg
    spread = mask(iota((rows, group), 0) // kdeg == iota((rows, group), 1))
    gather = mask(iota((group, rows), 0) == iota((group, rows), 1) // kdeg)
    for b in range(edge_ref.shape[0] // rows):
        sl = pl.ds(b * rows, rows)
        gl = pl.ds(b * group, group)
        edge = edge_ref[sl, :]
        pick = mask(iota((rows, at), 1) == index_ref[sl, :])
        pre = mm(edge, we[0]) + mm(pick, table[...]) + mm(spread, recv_ref[gl, :])
        msg = norm(mm(silu(pre).astype(BF), we[1])).astype(BF)
        if not last:
            out_edge[sl, :] = (edge.astype(F32) + msg.astype(F32)).astype(BF)
        agg[gl, :] = mm(gather, msg).astype(BF)
    new = node_update(mesh_ref[...], agg[...], wn)
    out_mesh[...] = new
    if not last:
        out_send[...] = mm(new, pe[0]).astype(BF)
        out_recv[...] = mm(new, pe[1]).astype(BF)


def call(kernel, at, args, outs, scratch, name, hbm=False):
    vmem = pl.BlockSpec(memory_space=pltpu.VMEM)
    return pl.pallas_call(
        kernel,
        in_specs=[pl.BlockSpec(memory_space=pltpu.SMEM)]
        + [pl.BlockSpec(memory_space=pl.ANY) if hbm else vmem] * len(args),
        out_specs=[vmem] * len(outs),
        out_shape=[jax.ShapeDtypeStruct(s, d) for s, d in outs],
        scratch_shapes=[pltpu.VMEM(*s) if isinstance(s, tuple) else s for s in scratch],
        compiler_params=pltpu.CompilerParams(vmem_limit_bytes=56 * 1024 * 1024),
        name=name,
    )(at, *args)


def swap(stack):
    return lax.ppermute(stack, "feat", [(0, 1), (1, 0)])


def ring(n, d):
    return [(i, (i + d) % n) for i in range(n)]


def stages(n):
    return (0, n // 2, n // 4, -(n // 4)), (0, n // 8, n // 16, -(n // 16)), tuple(range(n // 16))


def coarse_table(rows):
    n = lax.axis_size("region")
    far, mid, near = stages(n)
    for shifts in (far, mid):
        rows = jnp.concatenate(
            [rows] + [lax.ppermute(rows, "region", ring(n, d)) for d in shifts[1:]], axis=0
        )
    parts = [rows] + [lax.ppermute(rows, "region", ring(n, d)) for d in near[1:]]
    return parts + [swap(p) for p in parts]


def coarse_place(home):
    n = lax.axis_size("region")
    far, mid, near = stages(n)
    behind = (lax.axis_index("region") - home // 2) % n
    step = len(near)
    place_near = behind % step
    behind = behind - place_near
    part = n // 4
    place_mid = jnp.zeros_like(home)
    shift_mid = jnp.zeros_like(home)
    for k, d in enumerate(mid):
        here = behind % part == d % part
        place_mid = jnp.where(here, k, place_mid)
        shift_mid = jnp.where(here, d, shift_mid)
    behind = (behind - shift_mid) % n
    place_far = jnp.zeros_like(home)
    for k, d in enumerate(far):
        place_far = jnp.where(behind == d % n, k, place_far)
    other = (home % 2 != lax.axis_index("feat")).astype(I32)
    return ((other * step + place_near) * len(mid) + place_mid) * len(far) + place_far


def on_device(
    grid_lat, g2m_edge, g2m_src, g2m_owner, g2m_row, mesh_lat, m2m_edge, m2m_src,
    enc_edge_w, enc_node_w, proc_edge_w, proc_node_w,
):
    n = lax.axis_size("region")
    shards = lax.axis_size(AXES)
    myself = lax.axis_index(AXES)
    at = jnp.stack([lax.axis_index("region"), lax.axis_index("feat")]).astype(I32)
    grid_rows, width = grid_lat.shape
    mesh_rows = mesh_lat.shape[0]
    edges = g2m_edge.shape[0]
    cap = 2 * edges // shards
    layers = proc_edge_w.shape[0]
    mat = (width, width)

    enc_edge_o = swap(enc_edge_w)
    hold = limits(n, cap, edges)
    table = np.full((8, LANES), SPAN, np.int32)
    table[:2, 1 : 1 + len(hold)] = hold
    first = [hold[0], hold[0], 2 * cap]
    target_row = g2m_row.reshape(1, edges)
    slot, plain, heads = call(
        functools.partial(slots_kernel, n, cap, [-(-k // LANES) * LANES for k in first]), at,
        [g2m_owner.reshape(1, edges), target_row, jnp.asarray(table)],
        [((1, edges), I32), ((1, edges), I32), ((3, HEAD, width), BF)], [], "slots",
    )
    local_src = (g2m_src - myself * grid_rows).reshape(edges, 1)
    pack_args = [grid_lat, g2m_edge, local_src]
    half = width // 2
    packed = call(
        functools.partial(pack_kernel, [r * REGION for r in range(3)], False), at,
        [*pack_args, slot, heads, enc_edge_w, enc_edge_o],
        [((k + extra, half), BF) for k in first for extra in (2 * HEAD, 0)],
        [((2, *mat), BF), ((edges, width), BF)], "pack",
    )
    kdeg = m2m_src.shape[1]
    halo = mesh_rows // 2
    senders = m2m_src.reshape(mesh_rows * kdeg)
    home = senders // mesh_rows
    inside = senders % mesh_rows
    index = jnp.where(
        inside < MC_DEV,
        mesh_rows + 2 * halo + coarse_place(home) * MC_DEV + inside,
        senders - (myself * mesh_rows - halo),
    ).reshape(mesh_rows * kdeg, 1)
    arrivals, plan = [packed[4:]], [(0, True)]
    moving = [list(packed[:2]), list(packed[2:4])]
    for hop in range(1, n // 2 + 1):
        keep = hold[hop - 1]
        for way in range(2):
            moving[way] = [
                lax.ppermute(m[: keep + (2 * HEAD if k == 0 else 0)], "region", ring(n, 1 - 2 * way))
                for k, m in enumerate(moving[way])
            ]
            arrivals.append(moving[way])
            plan.append((2 * (n // 2 - hop), False))
    total = len(plan)
    span = -(-(total * (cap + 8) + 8) // 448) * 448
    mine, other = call(
        functools.partial(windows_kernel, n, cap, plan, [len(a) for a in arrivals]), at, sum(map(list, arrivals), []),
        [((span, width + LANES), BF)] * 2,
        [((total, 2 * HEAD, half), BF), ((2 * total, LANES), I32), pltpu.SMEM((2 * total, LANES), I32),
         pltpu.SemaphoreType.DMA((total, 4)), pltpu.SemaphoreType.DMA((total,)), pltpu.SemaphoreType.DMA],
        "windows", hbm=True,
    )
    theirs, index = lax.optimization_barrier((swap(other), index))
    enc_node_o = swap(enc_node_w)
    proc_edge_o = swap(proc_edge_w)
    proc_node_o = swap(proc_node_w)
    over = jnp.maximum(mine[span - 1, 0], theirs[span - 1, 0]) > 0

    def encode(*gots):
        return tuple(call(
            functools.partial(encode_kernel, len(gots)), at,
            [*gots, mesh_lat, enc_edge_w, enc_edge_o, enc_node_w, enc_node_o, proc_edge_w, proc_edge_o],
            [((mesh_rows, width), BF)] * 3,
            [((2, *mat), BF), ((3, *mat), BF), ((2, *mat), BF), ((mesh_rows, width), F32)], "encode",
        ))

    def padded():
        (sent,) = call(
            functools.partial(pack_kernel, None, True), at,
            [*pack_args, plain, target_row, enc_edge_w, enc_edge_o],
            [((shards * cap, width + LANES), BF)], [((2, *mat), BF), ((edges, width), BF)], "pack_padded",
        )
        got = lax.all_to_all(sent.reshape(shards, cap, width + LANES), AXES, split_axis=0, concat_axis=0, tiled=True)
        return encode(got.reshape(shards * cap, width + LANES))

    mesh, sender, receiver = lax.cond(over, padded, lambda: encode(mine, theirs))
    edge = m2m_edge.reshape(mesh_rows * kdeg, width)
    up = [(i, i + 1) for i in range(shards - 1)]
    for layer in range(layers):
        last = layer == layers - 1
        low = lax.ppermute(sender[mesh_rows - halo :], AXES, up)
        high = lax.ppermute(sender[:halo], AXES, [(b, a) for a, b in up])
        coarse = coarse_table(sender[:MC_DEV])
        args = [edge, index, sender, low, high, *coarse, receiver, mesh, proc_edge_w, proc_edge_o, proc_node_w, proc_node_o]
        outs = [((mesh_rows, width), BF)]
        scratch = [((2, *mat), BF), ((3, *mat), BF),
                   ((mesh_rows + 2 * halo + shards * MC_DEV, width), BF), ((mesh_rows, width), BF)]
        if not last:
            outs += [((mesh_rows * kdeg, width), BF)] + [((mesh_rows, width), BF)] * 2
            scratch += [((2, *mat), BF)]
        got = call(functools.partial(layer_kernel, kdeg, layer, last, len(coarse)), at, args, outs, scratch, "layer")
        mesh = got[0]
        if not last:
            edge, sender, receiver = got[1:]
    return mesh


def solution(mesh):
    rows = P(("ens", "region", "feat"))
    rows2 = P(("ens", "region", "feat"), None)
    return jax.shard_map(
        on_device,
        mesh=mesh,
        in_specs=(
            rows2, rows2, rows, rows2, rows, rows2,
            P(("ens", "region", "feat"), None, None), rows2,
            P(None, None, "feat"), P(None, None, "feat"),
            P(None, None, None, "feat"), P(None, None, None, "feat"),
        ),
        out_specs=rows2,
        check_vma=False,
    )
```
